64 devices in a mesh: dp: 4 (over x, y), sp: 16 (over z, core).
Axes of the slice: x: 2, y: 2, z: 8, core: 2. Of those that a mesh axis runs over, the one named last changes fastest.
The devices are a block of a 4x4x8 slice.
Arguments:
- q: bfloat16 [128, 32, 64], P('dp'), parts along dimension 0
- k: bfloat16 [128, 8192, 8, 64], P('dp', 'sp'), parts along dimension 0
- v: bfloat16 [128, 8192, 8, 64], P('dp', 'sp'), parts along dimension 0
Outputs:
- q: bfloat16 [128, 32, 64], P('dp'), parts along dimension 0
There are 4 independent parts. The reference program is written for one: setup_inputs(seed, part) draws one part's arguments, and reference() takes and returns one part's arrays. A program takes and returns all parts, laid end to end along the dimension named above; each array names one.
All inputs are finite; a program needn't handle non-finite values.
Results may differ from the reference program's by a relative error of at most 0.012.
Values are sent between devices in bfloat16 or wider.
A program may use at most 768 MiB of HBM per device.

```python
import jax
import jax.numpy as jnp

BATCH = 32
CACHE = 8192
HEADS = 32
KV_HEADS = 8
HEAD = 64


def setup_inputs(seed: int = 0, part: int = 0) -> dict:
    kq, kk, kv = (jax.random.fold_in(k, part) for k in jax.random.split(jax.random.key(seed), 3))
    return {
        "q": (3 * jax.random.normal(kq, (BATCH, HEADS, HEAD), jnp.float32)).astype(jnp.bfloat16),
        "k": jax.random.normal(kk, (BATCH, CACHE, KV_HEADS, HEAD), jnp.float32).astype(jnp.bfloat16),
        "v": jax.random.normal(kv, (BATCH, CACHE, KV_HEADS, HEAD), jnp.float32).astype(jnp.bfloat16),
    }


def einsum(form, a, b):
    return jnp.einsum(form, a.astype(jnp.float32), b.astype(jnp.float32))


def reference(q, k, v):
    grouped = q.reshape(BATCH, KV_HEADS, -1, HEAD)
    scores = einsum("bgsd,bugd->bgsu", grouped, k) * HEAD**-0.5
    weights = jax.nn.softmax(scores, -1).astype(jnp.bfloat16)
    return einsum("bgsu,bugd->bgsd", weights, v).astype(jnp.bfloat16).reshape(BATCH, HEADS, HEAD)
```

```python
import functools

import jax
import jax.numpy as jnp
from jax import lax
from jax.experimental import pallas as pl
from jax.experimental.pallas import tpu as pltpu
from jax.sharding import PartitionSpec as P

LOG2E = 1.4426950408889634
GROUP = 4
AHEAD = 8
MESH = pl.DeviceIdType.MESH


def iota(shape, dim):
    return lax.broadcasted_iota(jnp.int32, shape, dim)


def spread(q, rows, width):
    d = q.shape[1]
    wide = jnp.concatenate([q] * (width // d), axis=1)
    mine = iota(wide.shape, 0) % rows // (rows * d // width) == iota(wide.shape, 1) // d
    return jnp.where(mine, wide, jnp.zeros_like(wide))


def fold(halves, d):
    ys = []
    for o in halves:
        rows, width = o.shape
        mine = iota(o.shape, 0) // (rows * d // width) == iota(o.shape, 1) // d
        x = jnp.where(mine, o, 0.0)
        y = x[:, : 2 * d]
        for i in range(2 * d, width, 2 * d):
            y = y + x[:, i : i + 2 * d]
        ys.append(y + pltpu.roll(y, d, 1))
    return jnp.where(iota(ys[0].shape, 1) < d, ys[0], ys[1])


def as_row(columns, lanes):
    total = jnp.zeros((8, lanes), jnp.float32)
    at = iota(total.shape, 1) - iota(total.shape, 0)
    for i, column in enumerate(columns):
        for k in range(0, column.shape[0], 8):
            total = jnp.where(at == i * column.shape[0] + k, column[k : k + 8], total)
    return jnp.sum(total, axis=0, keepdims=True)


def kernel(n, q_ref, k_hbm, v_hbm, o_ref, kbuf, vbuf, pbuf, part, stat, got, gots, done, ksem, vsem, s_part, r_part, s_stat, r_stat, s_done, r_done):
    b = k_hbm.shape[0]
    d = q_ref.shape[2]
    rows = q_ref.shape[1] // 2
    lanes = 2 * d
    width = kbuf.shape[1] // 2
    me, dp = lax.axis_index("sp"), lax.axis_index("dp")
    others = sorted(range(1, n), key=lambda k: -min(k, n - k))
    to = {k: lax.rem(me + k, n) for k in others}
    frm = {k: lax.rem(me + n - k, n) for k in others}

    def keys(i):
        return pltpu.make_async_copy(k_hbm.at[i], kbuf.at[i], ksem.at[i])

    def values(i):
        return pltpu.make_async_copy(v_hbm.at[i], vbuf.at[i], vsem.at[i])

    for i in range(AHEAD):
        keys(i).start()
        values(i).start()
    barrier = pltpu.get_barrier_semaphore()
    for k in others:
        pl.semaphore_signal(barrier, inc=1, device_id=(dp, to[k]), device_id_type=MESH)

    def score(base):
        out = []
        for j in range(GROUP):
            q = spread(q_ref[base + j], rows, width)
            for h in range(2):
                out.append(jnp.dot(q[h * rows : (h + 1) * rows], kbuf[base + j, h * width : (h + 1) * width], preferred_element_type=jnp.float32))
        return out

    def soften(base, scores):
        for j in range(GROUP):
            ms, ls = [], []
            for h in range(2):
                s = scores[2 * j + h]
                m = jnp.max(s, axis=1, keepdims=True)
                p = jnp.exp2((s - m) * (d**-0.5 * LOG2E))
                pbuf[j, h * rows : (h + 1) * rows] = p.astype(jnp.bfloat16)
                ms.append(m * d**-0.5)
                ls.append(jnp.sum(p, axis=1, keepdims=True))
            stat[base + j] = as_row(ms + ls, lanes)

    def see(base):
        for j in range(GROUP):
            halves = [
                lax.dot_general(
                    pbuf[j, h * rows : (h + 1) * rows],
                    vbuf[base + j, h * width : (h + 1) * width],
                    (((1,), (1,)), ((), ())),
                    preferred_element_type=jnp.float32,
                )
                for h in range(2)
            ]
            part[base + j] = fold(halves, d).astype(jnp.bfloat16)

    def step(t, carry):
        base = t * GROUP
        for j in range(GROUP):
            i = base + j + AHEAD - GROUP

            @pl.when(i < b)
            def _():
                keys(i).start()
                values(i).start()

        for j in range(GROUP):
            keys(base + j).wait()
            values(base - GROUP + j).wait()
        scores = score(base)
        see(base - GROUP)
        soften(base, scores)
        return carry

    def part_copies(c, k, sender):
        src, dst = (me, to[k]) if sender else (frm[k], me)
        s = c * n + to[k]
        dev = dict(device_id=(dp, to[k]), device_id_type=MESH)
        return (
            pltpu.make_async_remote_copy(src_ref=part.at[s], dst_ref=got.at[c, src], send_sem=s_part.at[c, k], recv_sem=r_part.at[c, k], **dev),
            pltpu.make_async_remote_copy(src_ref=stat.at[s], dst_ref=gots.at[c, src], send_sem=s_stat.at[c, k], recv_sem=r_stat.at[c, k], **dev),
        )

    def done_copy(c, k, sender):
        src = me if sender else frm[k]
        return pltpu.make_async_remote_copy(
            src_ref=done.at[c * n + me],
            dst_ref=done.at[c * n + src],
            send_sem=s_done.at[c, k],
            recv_sem=r_done.at[c, k],
            device_id=(dp, to[k]),
            device_id_type=MESH,
        )

    def send_parts(c):
        for k in others:
            for copy in part_copies(c, k, True):
                copy.start()
        mine = c * n + me
        got[c, me] = part[mine]
        gots[c, me] = stat[mine]

    def put_together(c):
        for k in others:
            for copy in part_copies(c, k, False):
                copy.wait_recv()
        s = jnp.concatenate([gots[c, i] for i in range(n)], axis=0)
        e = jnp.exp(s - jnp.max(s, axis=0, keepdims=True))
        total = jnp.sum(e * pltpu.roll(s, lanes - 2 * rows, 1), axis=0, keepdims=True)
        f = e / total
        accs = []
        for k in range(0, rows, 8):
            at = iota((8, lanes), 1) // d * rows + k + iota((8, lanes), 0)
            acc = jnp.zeros((8, lanes), jnp.float32)
            for i in range(n):
                scale = jnp.take_along_axis(jnp.broadcast_to(f[i : i + 1], (8, lanes)), at, axis=1)
                acc += scale * got[c, i].astype(jnp.float32)[k : k + 8]
            accs.append(acc)
        done[c * n + me] = jnp.concatenate(accs, axis=0).astype(jnp.bfloat16)
        for k in others:
            done_copy(c, k, True).start()

    def lay_out(c):
        for k in others:
            done_copy(c, k, False).wait_recv()
        for i in range(n):
            x = done[c * n + i]
            o_ref[c * n + i, :rows] = x[:, :d]
            o_ref[c * n + i, rows:] = x[:, d:]

    for j in range(GROUP):
        keys(j).wait()
    soften(0, score(0))
    steps, chunks = b // GROUP, b // n
    t = 1
    for c in range(chunks - 1):
        upto = (c + 1) * n // GROUP + 1
        lax.fori_loop(t, upto, step, 0)
        t = upto
        if c == 0:
            pl.semaphore_wait(barrier, n - 1)
        send_parts(c)
    lax.fori_loop(t, steps, step, 0)
    for c in range(chunks - 1):
        put_together(c)
    for j in range(GROUP):
        values(b - GROUP + j).wait()
    see(b - GROUP)
    send_parts(chunks - 1)
    put_together(chunks - 1)
    for c in range(chunks):
        lay_out(c)
    for c in range(chunks):
        for k in others:
            for copy in part_copies(c, k, True):
                copy.wait_send()
            done_copy(c, k, True).wait_send()


def solution(mesh):
    n = mesh.shape["sp"]

    def step(q, k, v):
        b, u, g, d = k.shape
        heads = q.shape[1]
        rows, lanes = heads // 2, 2 * d
        k = jnp.transpose(k, (0, 2, 3, 1)).reshape(b, g * d, u)
        v = jnp.transpose(v, (0, 2, 3, 1)).reshape(b, g * d, u)
        c = b // n
        dma = pltpu.SemaphoreType.DMA
        return pl.pallas_call(
            functools.partial(kernel, n),
            out_shape=jax.ShapeDtypeStruct(q.shape, q.dtype),
            in_specs=[
                pl.BlockSpec(memory_space=pltpu.VMEM),
                pl.BlockSpec(memory_space=pl.ANY),
                pl.BlockSpec(memory_space=pl.ANY),
            ],
            out_specs=pl.BlockSpec(memory_space=pltpu.VMEM),
            scratch_shapes=[
                pltpu.VMEM((b, g * d, u), jnp.bfloat16),
                pltpu.VMEM((b, g * d, u), jnp.bfloat16),
                pltpu.VMEM((GROUP, heads, u), jnp.bfloat16),
                pltpu.VMEM((b, rows, lanes), jnp.bfloat16),
                pltpu.VMEM((b, 1, lanes), jnp.float32),
                pltpu.VMEM((c, n, rows, lanes), jnp.bfloat16),
                pltpu.VMEM((c, n, 1, lanes), jnp.float32),
                pltpu.VMEM((b, rows, lanes), jnp.bfloat16),
                dma((b,)),
                dma((b,)),
                dma((c, n)),
                dma((c, n)),
                dma((c, n)),
                dma((c, n)),
                dma((c, n)),
                dma((c, n)),
            ],
            compiler_params=pltpu.CompilerParams(collective_id=0, has_side_effects=True, vmem_limit_bytes=60 * 2**20),
        )(q, k, v)

    return jax.shard_map(
        step,
        mesh=mesh,
        in_specs=(P("dp", None, None), P("dp", "sp", None, None), P("dp", "sp", None, None)),
        out_specs=P("dp", None, None),
        check_vma=False,
    )
```

```python
import functools

import jax
import jax.numpy as jnp
from jax import lax
from jax.experimental import pallas as pl
from jax.experimental.pallas import tpu as pltpu
from jax.sharding import PartitionSpec as P

LOG2E = 1.4426950408889634
GROUP = 4
AHEAD = 2
MESH = pl.DeviceIdType.MESH


def iota(shape, dim):
    return lax.broadcasted_iota(jnp.int32, shape, dim)


def spread(q, rows, width):
    d = q.shape[1]
    wide = jnp.concatenate([q] * (width // d), axis=1)
    mine = iota(wide.shape, 0) % rows // (rows * d // width) == iota(wide.shape, 1) // d
    return jnp.where(mine, wide, jnp.zeros_like(wide))


def fold(halves, d):
    ys = []
    for o in halves:
        rows, width = o.shape
        mine = iota(o.shape, 0) // (rows * d // width) == iota(o.shape, 1) // d
        x = jnp.where(mine, o, 0.0)
        y = x[:, : 2 * d]
        for i in range(2 * d, width, 2 * d):
            y = y + x[:, i : i + 2 * d]
        ys.append(y + pltpu.roll(y, d, 1))
    return jnp.where(iota(ys[0].shape, 1) < d, ys[0], ys[1])


def as_row(columns, lanes):
    total = jnp.zeros((8, lanes), jnp.float32)
    at = iota(total.shape, 1) - iota(total.shape, 0)
    for i, column in enumerate(columns):
        for k in range(0, column.shape[0], 8):
            total = jnp.where(at == i * column.shape[0] + k, column[k : k + 8], total)
    return jnp.sum(total, axis=0, keepdims=True)


def kernel(n, q_hbm, k_hbm, v_hbm, done, q_ref, kbuf, vbuf, pbuf, part, stat, got, gots, qsem, ksem, vsem, s_part, r_part, s_stat, r_stat, s_done, r_done):
    b = k_hbm.shape[0]
    steps, chunks = b // GROUP, b // n
    d = q_ref.shape[2]
    rows = q_ref.shape[1] // 2
    lanes = 2 * d
    width = kbuf.shape[1] // 2
    me, dp = lax.axis_index("sp"), lax.axis_index("dp")
    others = sorted(range(1, n), key=lambda k: -min(k, n - k))
    to = {k: jnp.where(me + k < n, me + k, me + k - n) for k in others}

    def keys(t):
        at = pl.ds(t * GROUP, GROUP)
        return pltpu.make_async_copy(k_hbm.at[at], kbuf.at[at], ksem.at[t])

    def values(t):
        at = pl.ds(t * GROUP, GROUP)
        return pltpu.make_async_copy(v_hbm.at[at], vbuf.at[at], vsem.at[t])

    queries = pltpu.make_async_copy(q_hbm, q_ref, qsem)
    queries.start()
    keys(0).start()
    barrier = pltpu.get_barrier_semaphore()
    for k in others:
        pl.semaphore_signal(barrier, inc=1, device_id=(dp, to[k]), device_id_type=MESH)

    for t in range(AHEAD):
        keys(t + 1).start()
        values(t).start()

    def score(base):
        out = []
        for j in range(GROUP):
            q = spread(q_ref[base + j], rows, width)
            for h in range(2):
                out.append(jnp.dot(q[h * rows : (h + 1) * rows], kbuf[base + j, h * width : (h + 1) * width], preferred_element_type=jnp.float32))
        return out

    def soften(base, scores):
        for j in range(GROUP):
            ms, ls = [], []
            for h in range(2):
                s = scores[2 * j + h]
                m = jnp.max(s, axis=1, keepdims=True)
                p = jnp.exp2((s - m) * (d**-0.5 * LOG2E))
                pbuf[j, h * rows : (h + 1) * rows] = p.astype(jnp.bfloat16)
                ms.append(m * d**-0.5)
                ls.append(jnp.sum(p, axis=1, keepdims=True))
            stat[base + j] = as_row(ms + ls, lanes)

    def see(base):
        for j in range(GROUP):
            halves = [
                lax.dot_general(
                    pbuf[j, h * rows : (h + 1) * rows],
                    vbuf[base + j, h * width : (h + 1) * width],
                    (((1,), (1,)), ((), ())),
                    preferred_element_type=jnp.float32,
                )
                for h in range(2)
            ]
            part[base + j] = fold(halves, d).astype(jnp.bfloat16)

    def step(t, carry):
        base = t * GROUP

        @pl.when(t + AHEAD < steps)
        def _():
            keys(t + AHEAD).start()

        @pl.when(t - 1 + AHEAD < steps)
        def _():
            values(t - 1 + AHEAD).start()

        @pl.when(t == 2)
        def _():
            pl.semaphore_wait(barrier, n - 1)

        @pl.when(t >= 2)
        def _():
            send_parts(t - 2)

        keys(t).wait()
        values(t - 1).wait()
        scores = score(base)
        see(base - GROUP)
        soften(base, scores)
        return carry

    def owner(s):
        return s % GROUP * (n // GROUP) + s // GROUP % (n // GROUP)

    def owned(c):
        return c * n + me % (n // GROUP) * GROUP + me // (n // GROUP)

    def sending(src, dst, send_sem, recv_sem, dev):
        return pltpu.make_async_remote_copy(src_ref=src, dst_ref=dst, send_sem=send_sem, recv_sem=recv_sem, device_id=(dp, dev), device_id_type=MESH)

    def send_parts(t):
        for j in range(GROUP):
            s = t * GROUP + j
            c, dev = s // n, owner(s)

            @pl.when(dev != me)
            def _():
                sending(part.at[s], got.at[c, me], s_part, r_part.at[c], dev).start()
                sending(stat.at[s], gots.at[c, me], s_stat, r_stat.at[c], dev).start()

    def put_together(c):
        with jax.named_scope("parts"):
            some = pl.ds(0, n - 1)
            sending(got.at[c, some], got.at[c, some], s_part, r_part.at[c], me).wait_recv()
            sending(gots.at[c, some], gots.at[c, some], s_stat, r_stat.at[c], me).wait_recv()
        mine = owned(c)
        got[c, me] = part[mine]
        gots[c, me] = stat[mine]
        s = jnp.concatenate([gots[c, i] for i in range(n)], axis=0)
        e = jnp.exp(s - jnp.max(s, axis=0, keepdims=True))
        total = jnp.sum(e * pltpu.roll(s, lanes - 2 * rows, 1), axis=0, keepdims=True)
        f = e / total
        accs = []
        for k in range(0, rows, 8):
            at = iota((8, lanes), 1) // d * rows + k + iota((8, lanes), 0)
            acc = jnp.zeros((8, lanes), jnp.float32)
            for i in range(n):
                scale = jnp.take_along_axis(jnp.broadcast_to(f[i : i + 1], (8, lanes)), at, axis=1)
                acc += scale * got[c, i].astype(jnp.float32)[k : k + 8]
            accs.append(acc)
        done[mine] = jnp.concatenate(accs, axis=0).astype(jnp.bfloat16)
        for k in others:
            sending(done.at[mine], done.at[mine], s_done, r_done, to[k]).start()

    S = jax.named_scope
    with S("first"):
        queries.wait()
        keys(0).wait()
        soften(0, score(0))
    with S("loop"):
        lax.fori_loop(1, steps, step, 0)
    with S("send"):
        send_parts(steps - 2)
    with S("last"):
        values(steps - 1).wait()
        see(b - GROUP)
    with S("send"):
        send_parts(steps - 1)
    for c in range(chunks):
        put_together(c)
    with S("gather"):
        some = pl.ds(0, chunks * (n - 1))
        sending(done.at[some], done.at[some], s_done, r_done, me).wait_recv()
    with S("drain"):
        sending(done.at[some], done.at[some], s_done, r_done, me).wait_send()
        sending(part.at[some], part.at[some], s_part, r_part.at[0], me).wait_send()
        sending(stat.at[some], stat.at[some], s_stat, r_stat.at[0], me).wait_send()


def lay_out(x_ref, o_ref):
    rows, d = x_ref.shape[1], o_ref.shape[2]
    for i in range(x_ref.shape[0]):
        x = x_ref[i]
        o_ref[i, :rows] = x[:, :d]
        o_ref[i, rows:] = x[:, d:]


def solution(mesh):
    n = mesh.shape["sp"]

    def step(q, k, v):
        b, u, g, d = k.shape
        heads = q.shape[1]
        rows, lanes = heads // 2, 2 * d
        k = jnp.transpose(k, (0, 2, 3, 1)).reshape(b, g * d, u)
        v = jnp.transpose(v, (0, 2, 3, 1)).reshape(b, g * d, u)
        c = b // n
        dma = pltpu.SemaphoreType.DMA
        done = pl.pallas_call(
            functools.partial(kernel, n),
            out_shape=pltpu.VMEM((b, rows, lanes), q.dtype),
            in_specs=[
                pl.BlockSpec(memory_space=pltpu.HBM),
                pl.BlockSpec(memory_space=pltpu.HBM),
                pl.BlockSpec(memory_space=pltpu.HBM),
            ],
            out_specs=pl.BlockSpec(memory_space=pltpu.VMEM),
            scratch_shapes=[
                pltpu.VMEM(q.shape, q.dtype),
                pltpu.VMEM((b, g * d, u), jnp.bfloat16),
                pltpu.VMEM((b, g * d, u), jnp.bfloat16),
                pltpu.VMEM((GROUP, heads, u), jnp.bfloat16),
                pltpu.VMEM((b, rows, lanes), jnp.bfloat16),
                pltpu.VMEM((b, 1, lanes), jnp.float32),
                pltpu.VMEM((c, n, rows, lanes), jnp.bfloat16),
                pltpu.VMEM((c, n, 1, lanes), jnp.float32),
                dma,
                dma((b // GROUP,)),
                dma((b // GROUP,)),
                dma,
                dma((c,)),
                dma,
                dma((c,)),
                dma,
                dma,
            ],
            compiler_params=pltpu.CompilerParams(collective_id=0, has_side_effects=True, vmem_limit_bytes=60 * 2**20),
        )(q, k, v)
        return pl.pallas_call(
            lay_out,
            out_shape=jax.ShapeDtypeStruct(q.shape, q.dtype),
            in_specs=[pl.BlockSpec(memory_space=pltpu.VMEM)],
            out_specs=pl.BlockSpec(memory_space=pltpu.VMEM),
            compiler_params=pltpu.CompilerParams(vmem_limit_bytes=8 * 2**20),
        )(done)

    return jax.shard_map(
        step,
        mesh=mesh,
        in_specs=(P("dp", None, None), P("dp", "sp", None, None), P("dp", "sp", None, None)),
        out_specs=P("dp", None, None),
        check_vma=False,
    )
```

```python
import functools

import jax
import jax.numpy as jnp
from jax import lax
from jax.experimental import pallas as pl
from jax.experimental.pallas import tpu as pltpu
from jax.sharding import PartitionSpec as P

LOG2E = 1.4426950408889634
GROUP = 4
HUBS = 2
AHEAD = 2
MESH = pl.DeviceIdType.MESH


def iota(shape, dim):
    return lax.broadcasted_iota(jnp.int32, shape, dim)


def spread(q, rows, width):
    d = q.shape[1]
    wide = jnp.concatenate([q] * (width // d), axis=1)
    mine = iota(wide.shape, 0) % rows // (rows * d // width) == iota(wide.shape, 1) // d
    return jnp.where(mine, wide, jnp.zeros_like(wide))


def fold(halves, d):
    ys = []
    for o in halves:
        rows, width = o.shape
        mine = iota(o.shape, 0) // (rows * d // width) == iota(o.shape, 1) // d
        x = jnp.where(mine, o, 0.0)
        y = x[:, : 2 * d]
        for i in range(2 * d, width, 2 * d):
            y = y + x[:, i : i + 2 * d]
        ys.append(y + pltpu.roll(y, d, 1))
    return jnp.where(iota(ys[0].shape, 1) < d, ys[0], ys[1])


def as_row(columns, lanes):
    total = jnp.zeros((8, lanes), jnp.float32)
    at = iota(total.shape, 1) - iota(total.shape, 0)
    for i, column in enumerate(columns):
        for k in range(0, column.shape[0], 8):
            total = jnp.where(at == i * column.shape[0] + k, column[k : k + 8], total)
    return jnp.sum(total, axis=0, keepdims=True)


def kernel(n, q_hbm, k_hbm, v_hbm, done, q_ref, kbuf, vbuf, pbuf, part, stat, got, gots, qsem, ksem, vsem, s_part, r_part, s_stat, r_stat, s_done, r_done):
    b = k_hbm.shape[0]
    steps, chunks = b // GROUP, b // n
    d = q_ref.shape[2]
    rows = q_ref.shape[1] // 2
    lanes = 2 * d
    width = kbuf.shape[1] // 2
    me, dp = lax.axis_index("sp"), lax.axis_index("dp")
    others = sorted(range(1, n), key=lambda k: -min(k, n - k))
    to = {k: jnp.where(me + k < n, me + k, me + k - n) for k in others}

    def keys(t):
        at = pl.ds(t * GROUP, GROUP)
        return pltpu.make_async_copy(k_hbm.at[at], kbuf.at[at], ksem.at[t])

    def values(t):
        at = pl.ds(t * GROUP, GROUP)
        return pltpu.make_async_copy(v_hbm.at[at], vbuf.at[at], vsem.at[t])

    queries = pltpu.make_async_copy(q_hbm, q_ref, qsem)
    queries.start()
    keys(0).start()
    barrier = pltpu.get_barrier_semaphore()
    for k in others:
        pl.semaphore_signal(barrier, inc=1, device_id=(dp, to[k]), device_id_type=MESH)

    for t in range(AHEAD):
        keys(t + 1).start()
        values(t).start()

    def score(base):
        out = []
        for j in range(GROUP):
            q = spread(q_ref[base + j], rows, width)
            for h in range(2):
                out.append(jnp.dot(q[h * rows : (h + 1) * rows], kbuf[base + j, h * width : (h + 1) * width], preferred_element_type=jnp.float32))
        return out

    def soften(base, scores):
        for j in range(GROUP):
            ms, ls = [], []
            for h in range(2):
                s = scores[2 * j + h]
                m = jnp.max(s, axis=1, keepdims=True)
                p = jnp.exp2((s - m) * (d**-0.5 * LOG2E))
                pbuf[j, h * rows : (h + 1) * rows] = p.astype(jnp.bfloat16)
                ms.append(m * d**-0.5)
                ls.append(jnp.sum(p, axis=1, keepdims=True))
            stat[base + j] = as_row(ms + ls, lanes)

    def see(base):
        for j in range(GROUP):
            halves = [
                lax.dot_general(
                    pbuf[j, h * rows : (h + 1) * rows],
                    vbuf[base + j, h * width : (h + 1) * width],
                    (((1,), (1,)), ((), ())),
                    preferred_element_type=jnp.float32,
                )
                for h in range(2)
            ]
            part[base + j] = fold(halves, d).astype(jnp.bfloat16)

    def step(t, carry):
        base = t * GROUP

        @pl.when(t + AHEAD < steps)
        def _():
            keys(t + AHEAD).start()

        @pl.when(t - 1 + AHEAD < steps)
        def _():
            values(t - 1 + AHEAD).start()

        @pl.when(t == 2)
        def _():
            pl.semaphore_wait(barrier, n - 1)

        @pl.when(t >= 2)
        def _():
            send_parts(t - 2)

        keys(t).wait()
        values(t - 1).wait()
        scores = score(base)
        see(base - GROUP)
        soften(base, scores)
        return carry

    early = n // GROUP

    def owner(t, j):
        first = jnp.where(t < steps - 2, n // 4, 0)
        late = jnp.where(t == steps - 1, j % HUBS, first + j)
        slot = jnp.where(t == steps - 1, steps - 1 - early + 1 + j // HUBS, t - early + 1)
        return jnp.where(t < early, j * early + t, late), jnp.where(t < early, 0, slot)

    def sending(src, dst, send_sem, recv_sem, dev):
        return pltpu.make_async_remote_copy(src_ref=src, dst_ref=dst, send_sem=send_sem, recv_sem=recv_sem, device_id=(dp, dev), device_id_type=MESH)

    def send_parts(t):
        for j in range(GROUP):
            s = t * GROUP + j
            dev, slot = owner(t, j)

            @pl.when(dev != me)
            def _():
                sending(part.at[s], got.at[slot, me], s_part, r_part.at[slot], dev).start()
                sending(stat.at[s], gots.at[slot, me], s_stat, r_stat.at[slot], dev).start()

    def put_together(slot, mine):
        with jax.named_scope("parts"):
            some = pl.ds(0, n - 1)
            sending(got.at[slot, some], got.at[slot, some], s_part, r_part.at[slot], me).wait_recv()
            sending(gots.at[slot, some], gots.at[slot, some], s_stat, r_stat.at[slot], me).wait_recv()
        got[slot, me] = part[mine]
        gots[slot, me] = stat[mine]
        s = jnp.concatenate([gots[slot, i] for i in range(n)], axis=0)
        e = jnp.exp(s - jnp.max(s, axis=0, keepdims=True))
        total = jnp.sum(e * pltpu.roll(s, lanes - 2 * rows, 1), axis=0, keepdims=True)
        f = e / total
        accs = []
        for k in range(0, rows, 8):
            at = iota((8, lanes), 1) // d * rows + k + iota((8, lanes), 0)
            acc = jnp.zeros((8, lanes), jnp.float32)
            for i in range(n):
                scale = jnp.take_along_axis(jnp.broadcast_to(f[i : i + 1], (8, lanes)), at, axis=1)
                acc += scale * got[slot, i].astype(jnp.float32)[k : k + 8]
            accs.append(acc)
        done[mine] = jnp.concatenate(accs, axis=0).astype(jnp.bfloat16)
        for dev in range(n):

            @pl.when(dev != me)
            def _():
                sending(done.at[mine], done.at[mine], s_done, r_done, dev).start()

    S = jax.named_scope
    with S("first"):
        queries.wait()
        keys(0).wait()
        soften(0, score(0))
    with S("loop"):
        lax.fori_loop(1, steps, step, 0)
    with S("send"):
        send_parts(steps - 2)
    with S("last"):
        values(steps - 1).wait()
        see(b - GROUP)
    with S("send"):
        send_parts(steps - 1)
    put_together(0, me % early * GROUP + me // early)
    own = jnp.int32(1)
    for t in range(early, steps):
        for j in range(GROUP):
            if t < steps - 1 and j:
                continue
            if t < steps - 1:
                dev, slot = owner(t, 0)
                at = me - dev
                mine = (at >= 0) & (at < GROUP)
            else:
                dev, slot = owner(t, j)
                at, mine = j, dev == me
                if j % HUBS:
                    continue
                at = j + me
                mine = me < HUBS
            own = own + mine.astype(jnp.int32)
            slot = t - early + 1 if t < steps - 1 else steps - early + j // HUBS

            @pl.when(mine)
            def _():
                put_together(slot, t * GROUP + at)

    pool = got.reshape(got.shape[0] * n, rows, lanes)
    pools = gots.reshape(gots.shape[0] * n, 1, lanes)

    def pooled(count):
        return pool.at[pl.ds(0, count)]

    for c in range(1, 2 + GROUP):

        @pl.when(own == c)
        def _():
            with jax.named_scope("gather"):
                sending(pooled(b - c), pooled(b - c), s_done, r_done, me).wait_recv()
            with jax.named_scope("drain"):
                sending(pooled((n - 1) * c), pooled(b - c), s_done, r_done, me).wait_send()
                sending(pooled(b - c), pooled(b - c), s_part, r_part.at[0], me).wait_send()
                sending(pools.at[pl.ds(0, b - c)], pools.at[pl.ds(0, b - c)], s_stat, r_stat.at[0], me).wait_send()


def lay_out(x_ref, o_ref):
    rows, d = x_ref.shape[1], o_ref.shape[2]
    for i in range(x_ref.shape[0]):
        x = x_ref[i]
        o_ref[i, :rows] = x[:, :d]
        o_ref[i, rows:] = x[:, d:]


def solution(mesh):
    n = mesh.shape["sp"]

    def step(q, k, v):
        b, u, g, d = k.shape
        heads = q.shape[1]
        rows, lanes = heads // 2, 2 * d
        k = jnp.transpose(k, (0, 2, 3, 1)).reshape(b, g * d, u)
        v = jnp.transpose(v, (0, 2, 3, 1)).reshape(b, g * d, u)
        c = b // GROUP - n // GROUP + GROUP // HUBS
        dma = pltpu.SemaphoreType.DMA
        done = pl.pallas_call(
            functools.partial(kernel, n),
            out_shape=pltpu.VMEM((b, rows, lanes), q.dtype),
            in_specs=[
                pl.BlockSpec(memory_space=pltpu.HBM),
                pl.BlockSpec(memory_space=pltpu.HBM),
                pl.BlockSpec(memory_space=pltpu.HBM),
            ],
            out_specs=pl.BlockSpec(memory_space=pltpu.VMEM),
            scratch_shapes=[
                pltpu.VMEM(q.shape, q.dtype),
                pltpu.VMEM((b, g * d, u), jnp.bfloat16),
                pltpu.VMEM((b, g * d, u), jnp.bfloat16),
                pltpu.VMEM((GROUP, heads, u), jnp.bfloat16),
                pltpu.VMEM((b, rows, lanes), jnp.bfloat16),
                pltpu.VMEM((b, 1, lanes), jnp.float32),
                pltpu.VMEM((c, n, rows, lanes), jnp.bfloat16),
                pltpu.VMEM((c, n, 1, lanes), jnp.float32),
                dma,
                dma((b // GROUP,)),
                dma((b // GROUP,)),
                dma,
                dma((c,)),
                dma,
                dma((c,)),
                dma,
                dma,
            ],
            compiler_params=pltpu.CompilerParams(collective_id=0, has_side_effects=True, vmem_limit_bytes=60 * 2**20),
        )(q, k, v)
        return pl.pallas_call(
            lay_out,
            out_shape=jax.ShapeDtypeStruct(q.shape, q.dtype),
            in_specs=[pl.BlockSpec(memory_space=pltpu.VMEM)],
            out_specs=pl.BlockSpec(memory_space=pltpu.VMEM),
            compiler_params=pltpu.CompilerParams(vmem_limit_bytes=8 * 2**20),
        )(done)

    return jax.shard_map(
        step,
        mesh=mesh,
        in_specs=(P("dp", None, None), P("dp", "sp", None, None), P("dp", "sp", None, None)),
        out_specs=P("dp", None, None),
        check_vma=False,
    )
```

```python
import functools

import jax
import jax.numpy as jnp
from jax import lax
from jax.experimental import pallas as pl
from jax.experimental.pallas import tpu as pltpu
from jax.sharding import PartitionSpec as P

LOG2E = 1.4426950408889634
GROUP = 4
HUBS = 2
SLOTS = 4
AHEAD = 2
MESH = pl.DeviceIdType.MESH


def iota(shape, dim):
    return lax.broadcasted_iota(jnp.int32, shape, dim)


def spread(q, rows, width):
    d = q.shape[1]
    wide = jnp.concatenate([q] * (width // d), axis=1)
    mine = iota(wide.shape, 0) % rows // (rows * d // width) == iota(wide.shape, 1) // d
    return jnp.where(mine, wide, jnp.zeros_like(wide))


def fold(halves, d):
    ys = []
    for o in halves:
        rows, width = o.shape
        mine = iota(o.shape, 0) // (rows * d // width) == iota(o.shape, 1) // d
        x = jnp.where(mine, o, 0.0)
        y = x[:, : 2 * d]
        for i in range(2 * d, width, 2 * d):
            y = y + x[:, i : i + 2 * d]
        ys.append(y + pltpu.roll(y, d, 1))
    return jnp.where(iota(ys[0].shape, 1) < d, ys[0], ys[1])


def as_row(columns, lanes):
    total = jnp.zeros((8, lanes), jnp.float32)
    at = iota(total.shape, 1) - iota(total.shape, 0)
    for i, column in enumerate(columns):
        for k in range(0, column.shape[0], 8):
            total = jnp.where(at == i * column.shape[0] + k, column[k : k + 8], total)
    return jnp.sum(total, axis=0, keepdims=True)


def kernel(n, q_hbm, k_hbm, v_hbm, done, q_ref, kbuf, vbuf, pbuf, part, stat, got, gots, qsem, ksem, vsem, s_part, r_part, s_done, r_done):
    b = k_hbm.shape[0]
    steps, chunks = b // GROUP, b // n
    d = q_ref.shape[2]
    rows = q_ref.shape[1] // 2
    lanes = 2 * d
    width = kbuf.shape[1] // 2
    me, dp = lax.axis_index("sp"), lax.axis_index("dp")
    others = sorted(range(1, n), key=lambda k: -min(k, n - k))
    to = {k: jnp.where(me + k < n, me + k, me + k - n) for k in others}

    def keys(t):
        at = pl.ds(t * GROUP, GROUP)
        return pltpu.make_async_copy(k_hbm.at[at], kbuf.at[at], ksem.at[t % SLOTS])

    def values(t):
        at = pl.ds(t * GROUP, GROUP)
        return pltpu.make_async_copy(v_hbm.at[at], vbuf.at[at], vsem.at[t % SLOTS])

    queries = pltpu.make_async_copy(q_hbm, q_ref, qsem)
    queries.start()
    keys(0).start()
    barrier = pltpu.get_barrier_semaphore()
    for k in others:
        pl.semaphore_signal(barrier, inc=1, device_id=(dp, to[k]), device_id_type=MESH)

    for t in range(AHEAD):
        keys(t + 1).start()
        values(t).start()

    def score(base):
        out = []
        for j in range(GROUP):
            q = spread(q_ref[base + j], rows, width)
            for h in range(2):
                out.append(jnp.dot(q[h * rows : (h + 1) * rows], kbuf[base + j, h * width : (h + 1) * width], preferred_element_type=jnp.float32))
        return out

    def soften(base, scores):
        for j in range(GROUP):
            ms, ls = [], []
            for h in range(2):
                s = scores[2 * j + h]
                m = jnp.max(s, axis=1, keepdims=True)
                p = jnp.exp2((s - m) * (d**-0.5 * LOG2E))
                pbuf[j, h * rows : (h + 1) * rows] = p.astype(jnp.bfloat16)
                ms.append(m * d**-0.5)
                ls.append(jnp.sum(p, axis=1, keepdims=True))
            stat[base + j] = as_row(ms + ls, lanes)

    def see(base):
        for j in range(GROUP):
            halves = [
                lax.dot_general(
                    pbuf[j, h * rows : (h + 1) * rows],
                    vbuf[base + j, h * width : (h + 1) * width],
                    (((1,), (1,)), ((), ())),
                    preferred_element_type=jnp.float32,
                )
                for h in range(2)
            ]
            part[base + j] = fold(halves, d).astype(jnp.bfloat16)

    def step(t, carry):
        base = t * GROUP

        @pl.when(t + AHEAD < steps)
        def _():
            keys(t + AHEAD).start()

        @pl.when(t - 1 + AHEAD < steps)
        def _():
            values(t - 1 + AHEAD).start()

        @pl.when(t == 2)
        def _():
            pl.semaphore_wait(barrier, n - 1)

        @pl.when(t >= 2)
        def _():
            send_parts(t - 2)

        keys(t).wait()
        values(t - 1).wait()
        scores = score(base)
        see(base - GROUP)
        soften(base, scores)
        return carry

    pools = gots.reshape(gots.shape[0] * n, 1, lanes)
    early = n // GROUP

    def owner(t, j):
        first = jnp.where(t < steps - 2, n // 4, n - GROUP)
        late = jnp.where(t == steps - 1, j % HUBS, first + j)
        slot = jnp.where(t == steps - 1, steps - 1 - early + 1 + j // HUBS, t - early + 1)
        return jnp.where(t < early, j * early + t, late), jnp.where(t < early, 0, slot)

    def sending(src, dst, send_sem, recv_sem, dev):
        return pltpu.make_async_remote_copy(src_ref=src, dst_ref=dst, send_sem=send_sem, recv_sem=recv_sem, device_id=(dp, dev), device_id_type=MESH)

    def send_parts(t):
        for j in range(GROUP):
            s = t * GROUP + j
            dev, slot = owner(t, j)

            @pl.when(dev != me)
            def _():
                sending(part.at[s], got.at[slot, me], s_part, r_part.at[slot], dev).start()
                sending(stat.at[s], gots.at[slot, me], s_part, r_part.at[slot], dev).start()

    def put_together(slot, mine):
        with jax.named_scope("parts"):
            rest = pools.at[pl.ds(0, (n - 1) * (rows // 2 + 1))]
            sending(rest, rest, s_part, r_part.at[slot], me).wait_recv()
        got[slot, me] = part[mine]
        gots[slot, me] = stat[mine]
        s = jnp.concatenate([gots[slot, i] for i in range(n)], axis=0)
        e = jnp.exp(s - jnp.max(s, axis=0, keepdims=True))
        total = jnp.sum(e * pltpu.roll(s, lanes - 2 * rows, 1), axis=0, keepdims=True)
        f = e / total
        accs = []
        for k in range(0, rows, 8):
            at = iota((8, lanes), 1) // d * rows + k + iota((8, lanes), 0)
            acc = jnp.zeros((8, lanes), jnp.float32)
            for i in range(n):
                scale = jnp.take_along_axis(jnp.broadcast_to(f[i : i + 1], (8, lanes)), at, axis=1)
                acc += scale * got[slot, i].astype(jnp.float32)[k : k + 8]
            accs.append(acc)
        done[mine] = jnp.concatenate(accs, axis=0).astype(jnp.bfloat16)
        for dev in range(n):

            @pl.when(dev != me)
            def _():
                sending(done.at[mine], done.at[mine], s_done, r_done, dev).start()

    S = jax.named_scope
    with S("first"):
        queries.wait()
        keys(0).wait()
        soften(0, score(0))
    with S("loop"):
        lax.fori_loop(1, steps, step, 0)
    with S("send"):
        send_parts(steps - 2)
    with S("last"):
        values(steps - 1).wait()
        see(b - GROUP)
    with S("send"):
        send_parts(steps - 1)
    put_together(0, me % early * GROUP + me // early)
    own = jnp.int32(1)
    for t in range(early, steps):
        for j in range(GROUP):
            if t < steps - 1 and j:
                continue
            if t < steps - 1:
                dev, slot = owner(t, 0)
                at = me - dev
                mine = (at >= 0) & (at < GROUP)
            else:
                dev, slot = owner(t, j)
                at, mine = j, dev == me
                if j % HUBS:
                    continue
                at = j + me
                mine = me < HUBS
            own = own + mine.astype(jnp.int32)
            slot = t - early + 1 if t < steps - 1 else steps - early + j // HUBS

            @pl.when(mine)
            def _():
                put_together(slot, t * GROUP + at)

    pool = got.reshape(got.shape[0] * n, rows, lanes)

    def pooled(count):
        return pool.at[pl.ds(0, count)]

    for c in range(1, 2 + GROUP):

        @pl.when(own == c)
        def _():
            with jax.named_scope("gather"):
                sending(pooled(b - c), pooled(b - c), s_done, r_done, me).wait_recv()
            with jax.named_scope("drain"):
                sending(pooled((n - 1) * c), pooled(b - c), s_done, r_done, me).wait_send()
                rest = pools.at[pl.ds(0, (b - c) * (rows // 2 + 1))]
                sending(rest, rest, s_part, r_part.at[0], me).wait_send()


def lay_out(x_ref, o_ref):
    rows, d = x_ref.shape[1], o_ref.shape[2]
    for i in range(x_ref.shape[0]):
        x = x_ref[i]
        o_ref[i, :rows] = x[:, :d]
        o_ref[i, rows:] = x[:, d:]


def solution(mesh):
    n = mesh.shape["sp"]

    def step(q, k, v):
        b, u, g, d = k.shape
        heads = q.shape[1]
        rows, lanes = heads // 2, 2 * d
        k = jnp.transpose(k, (0, 2, 3, 1)).reshape(b, g * d, u)
        v = jnp.transpose(v, (0, 2, 3, 1)).reshape(b, g * d, u)
        c = b // GROUP - n // GROUP + GROUP // HUBS
        dma = pltpu.SemaphoreType.DMA
        done = pl.pallas_call(
            functools.partial(kernel, n),
            out_shape=pltpu.VMEM((b, rows, lanes), q.dtype),
            in_specs=[
                pl.BlockSpec(memory_space=pltpu.HBM),
                pl.BlockSpec(memory_space=pltpu.HBM),
                pl.BlockSpec(memory_space=pltpu.HBM),
            ],
            out_specs=pl.BlockSpec(memory_space=pltpu.VMEM),
            scratch_shapes=[
                pltpu.VMEM(q.shape, q.dtype),
                pltpu.VMEM((b, g * d, u), jnp.bfloat16),
                pltpu.VMEM((b, g * d, u), jnp.bfloat16),
                pltpu.VMEM((GROUP, heads, u), jnp.bfloat16),
                pltpu.VMEM((b, rows, lanes), jnp.bfloat16),
                pltpu.VMEM((b, 1, lanes), jnp.float32),
                pltpu.VMEM((c, n, rows, lanes), jnp.bfloat16),
                pltpu.VMEM((-(-b * (rows // 2 + 1) // n), n, 1, lanes), jnp.float32),
                dma,
                dma((SLOTS,)),
                dma((SLOTS,)),
                dma,
                dma((c,)),
                dma,
                dma,
            ],
            compiler_params=pltpu.CompilerParams(collective_id=0, has_side_effects=True, vmem_limit_bytes=60 * 2**20),
        )(q, k, v)
        return pl.pallas_call(
            lay_out,
            out_shape=jax.ShapeDtypeStruct(q.shape, q.dtype),
            in_specs=[pl.BlockSpec(memory_space=pltpu.VMEM)],
            out_specs=pl.BlockSpec(memory_space=pltpu.VMEM),
            compiler_params=pltpu.CompilerParams(vmem_limit_bytes=8 * 2**20),
        )(done)

    return jax.shard_map(
        step,
        mesh=mesh,
        in_specs=(P("dp", None, None), P("dp", "sp", None, None), P("dp", "sp", None, None)),
        out_specs=P("dp", None, None),
        check_vma=False,
    )
```

```python
import functools

import jax
import jax.numpy as jnp
from jax import lax
from jax.experimental import pallas as pl
from jax.experimental.pallas import tpu as pltpu
from jax.sharding import PartitionSpec as P

LOG2E = 1.4426950408889634
GROUP = 4
HUBS = 2
SLOTS = 4
AHEAD = 2
MESH = pl.DeviceIdType.MESH


def iota(shape, dim):
    return lax.broadcasted_iota(jnp.int32, shape, dim)


def spread(q, rows, width):
    d = q.shape[1]
    wide = jnp.concatenate([q] * (width // d), axis=1)
    mine = iota(wide.shape, 0) % rows // (rows * d // width) == iota(wide.shape, 1) // d
    return jnp.where(mine, wide, jnp.zeros_like(wide))


def fold(halves, d):
    ys = []
    for o in halves:
        rows, width = o.shape
        mine = iota(o.shape, 0) // (rows * d // width) == iota(o.shape, 1) // d
        x = jnp.where(mine, o, 0.0)
        y = x[:, : 2 * d]
        for i in range(2 * d, width, 2 * d):
            y = y + x[:, i : i + 2 * d]
        ys.append(y + pltpu.roll(y, d, 1))
    return jnp.where(iota(ys[0].shape, 1) < d, ys[0], ys[1])


def as_row(columns, lanes):
    total = jnp.zeros((8, lanes), jnp.float32)
    at = iota(total.shape, 1) - iota(total.shape, 0)
    for i, column in enumerate(columns):
        for k in range(0, column.shape[0], 8):
            total = jnp.where(at == i * column.shape[0] + k, column[k : k + 8], total)
    return jnp.sum(total, axis=0, keepdims=True)


def kernel(n, q_hbm, k_hbm, v_hbm, done, q_ref, kbuf, vbuf, pbuf, part, stat, got, gots, qsem, ksem, vsem, s_part, r_part, s_done, r_done):
    b = k_hbm.shape[0]
    steps, chunks = b // GROUP, b // n
    d = q_ref.shape[2]
    rows = q_ref.shape[1] // 2
    lanes = 2 * d
    width = kbuf.shape[1] // 2
    me, dp = lax.axis_index("sp"), lax.axis_index("dp")
    others = sorted(range(1, n), key=lambda k: -min(k, n - k))
    to = {k: jnp.where(me + k < n, me + k, me + k - n) for k in others}

    def keys(t):
        at = pl.ds(t * GROUP, GROUP)
        return pltpu.make_async_copy(k_hbm.at[at], kbuf.at[at], ksem.at[t % SLOTS])

    def values(t):
        at = pl.ds(t * GROUP, GROUP)
        return pltpu.make_async_copy(v_hbm.at[at], vbuf.at[at], vsem.at[t % SLOTS])

    queries = pltpu.make_async_copy(q_hbm, q_ref, qsem)
    queries.start()
    keys(0).start()
    barrier = pltpu.get_barrier_semaphore()
    for k in others:
        pl.semaphore_signal(barrier, inc=1, device_id=(dp, to[k]), device_id_type=MESH)

    for t in range(AHEAD):
        keys(t + 1).start()
        values(t).start()

    def score(base):
        out = []
        for j in range(GROUP):
            q = spread(q_ref[base + j], rows, width)
            for h in range(2):
                out.append(jnp.dot(q[h * rows : (h + 1) * rows], kbuf[base + j, h * width : (h + 1) * width], preferred_element_type=jnp.float32))
        return out

    def soften(base, scores):
        for j in range(GROUP):
            ms, ls = [], []
            for h in range(2):
                s = scores[2 * j + h]
                m = jnp.max(s, axis=1, keepdims=True)
                p = jnp.exp2((s - m) * (d**-0.5 * LOG2E))
                pbuf[j, h * rows : (h + 1) * rows] = p.astype(jnp.bfloat16)
                ms.append(m * d**-0.5)
                ls.append(jnp.sum(p, axis=1, keepdims=True))
            stat[base + j] = as_row(ms + ls, lanes)

    def see(base):
        for j in range(GROUP):
            halves = [
                lax.dot_general(
                    pbuf[j, h * rows : (h + 1) * rows],
                    vbuf[base + j, h * width : (h + 1) * width],
                    (((1,), (1,)), ((), ())),
                    preferred_element_type=jnp.float32,
                )
                for h in range(2)
            ]
            part[base + j] = fold(halves, d).astype(jnp.bfloat16)

    def step(t, carry):
        base = t * GROUP

        @pl.when(t + AHEAD < steps)
        def _():
            keys(t + AHEAD).start()

        @pl.when(t - 1 + AHEAD < steps)
        def _():
            values(t - 1 + AHEAD).start()

        @pl.when(t == 2)
        def _():
            pl.semaphore_wait(barrier, n - 1)

        @pl.when(t >= 2)
        def _():
            send_parts(t - 2)

        keys(t).wait()
        values(t - 1).wait()
        scores = score(base)
        see(base - GROUP)
        soften(base, scores)
        return carry

    pools = gots.reshape(gots.shape[0] * n, 1, lanes)
    early = n // GROUP

    def owner(t, j):
        first = jnp.where(t < steps - 2, n // 4, n - GROUP)
        late = jnp.where(t == steps - 1, j % HUBS, first + j)
        slot = jnp.where(t == steps - 1, steps - 1 - early + 1 + j // HUBS, t - early + 1)
        return jnp.where(t < early, j * early + t, late), jnp.where(t < early, 0, slot)

    def sending(src, dst, send_sem, recv_sem, dev):
        return pltpu.make_async_remote_copy(src_ref=src, dst_ref=dst, send_sem=send_sem, recv_sem=recv_sem, device_id=(dp, dev), device_id_type=MESH)

    def send_parts(t):
        for j in range(GROUP):
            s = t * GROUP + j
            dev, slot = owner(t, j)

            @pl.when(dev != me)
            def _():
                sending(part.at[s], got.at[slot, me], s_part, r_part.at[slot], dev).start()
                sending(stat.at[s], gots.at[slot, me], s_part, r_part.at[slot], dev).start()

    def put_together(slot, mine):
        with jax.named_scope("parts"):
            rest = pools.at[pl.ds(0, (n - 1) * (rows // 2 + 1))]
            sending(rest, rest, s_part, r_part.at[slot], me).wait_recv()
        got[slot, me] = part[mine]
        gots[slot, me] = stat[mine]
        s = jnp.concatenate([gots[slot, i] for i in range(n)], axis=0)
        e = jnp.exp(s - jnp.max(s, axis=0, keepdims=True))
        total = jnp.sum(e * pltpu.roll(s, lanes - 2 * rows, 1), axis=0, keepdims=True)
        f = e / total
        accs = []
        for k in range(0, rows, 8):
            at = iota((8, lanes), 1) // d * rows + k + iota((8, lanes), 0)
            acc = jnp.zeros((8, lanes), jnp.float32)
            for i in range(n):
                scale = jnp.take_along_axis(jnp.broadcast_to(f[i : i + 1], (8, lanes)), at, axis=1)
                acc += scale * got[slot, i].astype(jnp.float32)[k : k + 8]
            accs.append(acc)
        done[mine] = jnp.concatenate(accs, axis=0).astype(jnp.bfloat16)
        for dev in range(n):

            @pl.when(dev != me)
            def _():
                sending(done.at[mine], done.at[mine], s_done, r_done, dev).start()

    S = jax.named_scope
    with S("first"):
        queries.wait()
        keys(0).wait()
        soften(0, score(0))
    with S("loop"):
        lax.fori_loop(1, steps, step, 0)
    with S("send"):
        send_parts(steps - 2)
    with S("last"):
        values(steps - 1).wait()
        see(b - GROUP)
    with S("send"):
        send_parts(steps - 1)
    put_together(0, me % early * GROUP + me // early)
    own = jnp.int32(1)
    for t in range(early, steps):
        for j in range(GROUP):
            if t < steps - 1 and j:
                continue
            if t < steps - 1:
                dev, slot = owner(t, 0)
                at = me - dev
                mine = (at >= 0) & (at < GROUP)
            else:
                dev, slot = owner(t, j)
                at, mine = j, dev == me
                if j % HUBS:
                    continue
                at = j + me
                mine = me < HUBS
            own = own + mine.astype(jnp.int32)
            slot = t - early + 1 if t < steps - 1 else steps - early + j // HUBS

            @pl.when(mine)
            def _():
                put_together(slot, t * GROUP + at)

    pool = got.reshape(got.shape[0] * n, rows, lanes)

    def pooled(count):
        return pool.at[pl.ds(0, count)]

    for c in range(1, 2 + GROUP):

        @pl.when(own == c)
        def _():
            with jax.named_scope("gather"):
                sending(pooled(b - c), pooled(b - c), s_done, r_done, me).wait_recv()
            with jax.named_scope("drain"):
                sending(pooled((n - 1) * c), pooled(b - c), s_done, r_done, me).wait_send()
                rest = pools.at[pl.ds(0, (b - c) * (rows // 2 + 1))]
                sending(rest, rest, s_part, r_part.at[0], me).wait_send()


def lay_out(x_ref, o_hbm, o_ref, sem):
    rows, d = x_ref.shape[1], o_ref.shape[2]
    per = x_ref.shape[0] // 4
    copies = []
    for c in range(4):
        for i in range(c * per, (c + 1) * per):
            x = x_ref[i]
            o_ref[i, :rows] = x[:, :d]
            o_ref[i, rows:] = x[:, d:]
        at = pl.ds(c * per, per)
        copies.append(pltpu.make_async_copy(o_ref.at[at], o_hbm.at[at], sem.at[c]))
        copies[-1].start()
    for copy in copies:
        copy.wait()


def solution(mesh):
    n = mesh.shape["sp"]

    def step(q, k, v):
        b, u, g, d = k.shape
        heads = q.shape[1]
        rows, lanes = heads // 2, 2 * d
        k = jnp.transpose(k, (0, 2, 3, 1)).reshape(b, g * d, u)
        v = jnp.transpose(v, (0, 2, 3, 1)).reshape(b, g * d, u)
        c = b // GROUP - n // GROUP + GROUP // HUBS
        dma = pltpu.SemaphoreType.DMA
        done = pl.pallas_call(
            functools.partial(kernel, n),
            out_shape=pltpu.VMEM((b, rows, lanes), q.dtype),
            in_specs=[
                pl.BlockSpec(memory_space=pltpu.HBM),
                pl.BlockSpec(memory_space=pltpu.HBM),
                pl.BlockSpec(memory_space=pltpu.HBM),
            ],
            out_specs=pl.BlockSpec(memory_space=pltpu.VMEM),
            scratch_shapes=[
                pltpu.VMEM(q.shape, q.dtype),
                pltpu.VMEM((b, g * d, u), jnp.bfloat16),
                pltpu.VMEM((b, g * d, u), jnp.bfloat16),
                pltpu.VMEM((GROUP, heads, u), jnp.bfloat16),
                pltpu.VMEM((b, rows, lanes), jnp.bfloat16),
                pltpu.VMEM((b, 1, lanes), jnp.float32),
                pltpu.VMEM((c, n, rows, lanes), jnp.bfloat16),
                pltpu.VMEM((-(-b * (rows // 2 + 1) // n), n, 1, lanes), jnp.float32),
                dma,
                dma((SLOTS,)),
                dma((SLOTS,)),
                dma,
                dma((c,)),
                dma,
                dma,
            ],
            compiler_params=pltpu.CompilerParams(collective_id=0, has_side_effects=True, vmem_limit_bytes=60 * 2**20),
        )(q, k, v)
        return pl.pallas_call(
            lay_out,
            out_shape=jax.ShapeDtypeStruct(q.shape, q.dtype),
            in_specs=[pl.BlockSpec(memory_space=pltpu.VMEM)],
            out_specs=pl.BlockSpec(memory_space=pltpu.HBM),
            scratch_shapes=[pltpu.VMEM(q.shape, q.dtype), pltpu.SemaphoreType.DMA((4,))],
            compiler_params=pltpu.CompilerParams(vmem_limit_bytes=8 * 2**20),
        )(done)

    return jax.shard_map(
        step,
        mesh=mesh,
        in_specs=(P("dp", None, None), P("dp", "sp", None, None), P("dp", "sp", None, None)),
        out_specs=P("dp", None, None),
        check_vma=False,
    )
```
